256 devices in a mesh: fsdp: 64 (over z, x, core), tp: 4 (over y).
Axes of the slice: x: 4, y: 4, z: 8, core: 2. Of those that a mesh axis runs over, the one named last changes fastest.
Arguments:
- master: float32 [2048, 8192], P('fsdp', 'tp'), may hold values from -0.0625 to 0.0625
- first_moment: float32 [2048, 8192], P('fsdp', 'tp'), may hold values from -0.0029296875 to 0.0029296875
- second_moment: float32 [2048, 8192], P('fsdp', 'tp'), may hold values from 2.9802322e-08 to 1.1920929e-06
- gradients: float32 [2048, 8192], P('fsdp', 'tp'), as said below
- step_count: int32 [1], replicated, may hold values from 1 to 8
- tile_round: int32 [256], replicated, may hold values from 0 to 3, as said below
Outputs:
- new_master: float32 [2048, 8192], P('fsdp', 'tp')
- new_first: float32 [2048, 8192], P('fsdp', 'tp')
- new_second: float32 [2048, 8192], P('fsdp', 'tp')
- weights: bfloat16 [2048, 8192], P(None, 'tp')
The draws below stay inside these ranges and needn't reach their ends.
Inputs may be any that keep to these rules, and one draw needn't show every extreme that they name: `tile_round`: each aligned block of 4 entries (the tiles of one index of fsdp) holds every round number 0 to 3 exactly once. `gradients`: exactly one entry has magnitude 1000 or more; every other entry has magnitude under 100, and in every round without that entry the sum of squares is under 1e5.
All inputs are finite; a program needn't handle non-finite values.
Results may differ from the reference program's by a relative error of at most 0.001.
Values may be sent and summed in bfloat16 or wider, within the bound.
No kernel may reach another device: no remote copies, remote signals or barrier semaphores. Data moves between devices by JAX's collectives and lax.ppermute only.
A program may use at most 64 MiB of HBM per device.

```python
import math
import jax
import jax.numpy as jnp

COLS = 8192
TILE_ROWS = 8
ROUNDS = 4
ROWS_DEV = 32
ROWS = 2048
TILES = 256


def round_labels(key):
    blocks = ROWS // ROWS_DEV
    scores = jax.random.randint(jax.random.fold_in(key, 7), (blocks, ROUNDS), 0, 2 ** 30)
    order = jnp.argsort(scores, axis=1, stable=True).astype(jnp.int32)
    return order.reshape(TILES)


def draw_gradients(key, part):
    labels = round_labels(key)
    keys = jax.random.split(jax.random.fold_in(key, 29), 7)
    base = jax.random.normal(keys[0], (ROWS, COLS), jnp.float32)
    row_scale = jnp.exp(jax.random.uniform(keys[1], (ROWS, 1), jnp.float32, 0.0, math.log(10.0)))
    low_lo, low_hi, high_lo, high_hi = (0.05, 0.5, 2.0, 40.0)
    row_ids = jnp.arange(ROWS, dtype=jnp.int32).reshape(ROWS, 1)
    col_ids = jnp.arange(COLS, dtype=jnp.int32).reshape(1, COLS)
    blocks = ROWS // ROWS_DEV
    row_rise = 1.0 + 2.0 * (row_ids // ROWS_DEV).astype(jnp.float32) / max(blocks - 1, 1)
    col_rise = 1.0 + 2.0 * col_ids.astype(jnp.float32) / max(COLS - 1, 1)
    values = base * row_scale * row_rise * col_rise
    row_round = jnp.repeat(labels, TILE_ROWS).reshape(ROWS, 1)
    onehot = (row_round == jnp.arange(ROUNDS, dtype=jnp.int32).reshape(1, ROUNDS)).astype(jnp.float32)
    row_squares = jnp.sum(values * values, axis=1)
    round_squares = jnp.sum(onehot * row_squares.reshape(ROWS, 1), axis=0)
    shuffled = jax.random.permutation(keys[5], ROUNDS)
    is_low = shuffled < ROUNDS // 2
    fraction = jax.random.uniform(keys[6], (ROUNDS,), jnp.float32, 0.0, 1.0)
    low_target = jnp.exp(math.log(low_lo) + fraction * (math.log(low_hi) - math.log(low_lo)))
    high_target = jnp.exp(math.log(high_lo) + fraction * (math.log(high_hi) - math.log(high_lo)))
    target = jnp.where(is_low, low_target, high_target)
    factor = jnp.sqrt(target / round_squares)
    row_factor = jnp.sum(onehot * factor.reshape(1, ROUNDS), axis=1)
    values = values * row_factor.reshape(ROWS, 1)
    pick_row = jax.random.randint(keys[2], (), 0, ROWS)
    pick_col = jax.random.randint(keys[3], (), 0, COLS)
    spot = jnp.logical_and(row_ids == pick_row, col_ids == pick_col)
    return jnp.where(spot, jnp.float32(5000.0), values).astype(jnp.float32)


def draw_tile_round(key, part):
    return round_labels(key)


def steps_of(rng, extent, cuts, smallest, high):
    loudness, own = 1.0, jax.random.fold_in(rng, 6)
    for position, shards_of in cuts:
        draws = jnp.exp(jax.random.uniform(jax.random.fold_in(own, position), (shards_of,), jnp.float32, smallest / len(cuts), high / len(cuts)))
        loudness = loudness * jnp.repeat(draws, extent[position] // shards_of).reshape([-1 if axis == position else 1 for axis in range(len(extent))])
    return loudness


def normal_values(own_key, shape, deviation, limit, shards=(), kind=jnp.bfloat16):
    gain = steps_of(own_key, shape, shards, -0.22, 0.18) if shards else 1.0
    array = jax.random.normal(own_key, shape, jnp.float32) * deviation * gain
    return jnp.minimum(jnp.maximum(array, -limit), limit).astype(kind)


def setup_inputs(seed: int = 0) -> dict:
    key_list = jax.random.split(jax.random.key(seed), 7)
    return {
        "master": normal_values(key_list[0], (ROWS, COLS), COLS ** -0.5, 0.0625, ((0, 64), (1, 4)), jnp.float32),
        "first_moment": normal_values(key_list[1], (ROWS, COLS), (2.0 * (ROWS * COLS) ** (-0.5)), 0.0029296875, ((0, 64), (1, 4)), jnp.float32),
        "second_moment": jnp.clip(jnp.exp(math.log(1.1920928955078125e-06) - 3.6888795 * jax.random.uniform(key_list[2], (ROWS, COLS), jnp.float32) ** steps_of(key_list[2], (ROWS, COLS), ((0, 64), (1, 4)), -0.2, 0.2)), 2.9802322387695312e-08, 1.1920928955078125e-06),
        "gradients": draw_gradients(jax.random.fold_in(key_list[6], 71), 0),
        "step_count": jax.random.randint(key_list[4], (1,), 1, 9).astype(jnp.int32),
        "tile_round": draw_tile_round(jax.random.fold_in(key_list[6], 71), 0),
    }


beta_one = 0.9
beta_two = 0.95
adam_epsilon = 1e-08
learning_rate = 0.01
weight_decay = 0.1
clip_norm = 1.0
overflow_limit = 1000.0

def reference(master, first_moment, second_moment, gradients, step_count, tile_round):
    row_count, columns = master.shape
    tile_count = tile_round.shape[0]
    shaped = (tile_count, row_count // tile_count, columns)
    params = master.reshape(shaped)
    moment_one = first_moment.reshape(shaped)
    moment_two = second_moment.reshape(shaped)
    grads = gradients.reshape(shaped)
    labels = tile_round.reshape(tile_count, 1, 1)
    steps = step_count[0].astype(jnp.float32)
    correct_one = 1.0 - jnp.power(jnp.float32(beta_one), steps)
    correct_two = 1.0 - jnp.power(jnp.float32(beta_two), steps)
    out_p, out_m, out_v = (params, moment_one, moment_two)
    for round_index in range(ROUNDS):
        inside = labels == round_index
        total = jnp.sum(jnp.where(inside, grads * grads, jnp.float32(0.0)))
        overflow = jnp.logical_and(inside, jnp.abs(grads) >= overflow_limit)
        broken = jnp.max(jnp.where(overflow, jnp.int32(1), jnp.int32(0)))
        scale = jnp.minimum(jnp.float32(1.0), clip_norm / (jnp.sqrt(total) + 1e-06))
        clipped = grads * scale
        moment_new = beta_one * moment_one + (1.0 - beta_one) * clipped
        second_new = beta_two * moment_two + (1.0 - beta_two) * clipped * clipped
        ratio = moment_new / correct_one / (jnp.sqrt(second_new / correct_two) + adam_epsilon)
        param_new = params - learning_rate * (ratio + weight_decay * params)
        apply = jnp.logical_and(inside, broken == 0)
        out_p = jnp.where(apply, param_new, out_p)
        out_m = jnp.where(apply, moment_new, out_m)
        out_v = jnp.where(apply, second_new, out_v)
    new_master = out_p.reshape(row_count, columns)
    return (new_master, out_m.reshape(row_count, columns), out_v.reshape(row_count, columns), new_master.astype(jnp.bfloat16))
```

```python
import jax
import jax.numpy as jnp
from jax import lax
from jax.sharding import Mesh
from jax.sharding import PartitionSpec as P

ROUNDS = 4
FSDP = ("z", "x", "core")
ALL = ("z", "x", "core", "tp")


beta_one = 0.9
beta_two = 0.95
adam_epsilon = 1e-08
learning_rate = 0.01
weight_decay = 0.1
clip_norm = 1.0
square_limit = 1000000.0


def sum_over_devices(value, devices):
    copies = jnp.broadcast_to(value, (devices,) + value.shape)
    return jnp.sum(lax.all_to_all(copies, ALL, 0, 0, tiled=True), axis=0)


def local(devices, master, first_moment, second_moment, gradients, step_count, tile_round):
    row_count, columns = master.shape
    shaped = (ROUNDS, row_count // ROUNDS, columns)
    params = master.reshape(shaped)
    moment_one = first_moment.reshape(shaped)
    moment_two = second_moment.reshape(shaped)
    grads = gradients.reshape(shaped)
    mine = lax.dynamic_slice_in_dim(tile_round, lax.axis_index(FSDP) * ROUNDS, ROUNDS)
    is_round = mine[None, :] == jnp.arange(ROUNDS, dtype=jnp.int32)[:, None]
    squares = jnp.sum(grads * grads, axis=(1, 2))
    totals = sum_over_devices(
        jnp.sum(jnp.where(is_round, squares[None, :], 0.0), axis=1), devices
    )
    total_of_slot = jnp.sum(jnp.where(is_round, totals[:, None], 0.0), axis=0)
    total_of_slot = total_of_slot.reshape(ROUNDS, 1, 1)
    scale = jnp.minimum(jnp.float32(1.0), clip_norm / (jnp.sqrt(total_of_slot) + 1e-06))
    keeping = total_of_slot >= square_limit
    steps = step_count[0].astype(jnp.float32)
    correct_one = 1.0 - jnp.power(jnp.float32(beta_one), steps)
    correct_two = 1.0 - jnp.power(jnp.float32(beta_two), steps)
    clipped = grads * scale
    moment_new = beta_one * moment_one + (1.0 - beta_one) * clipped
    second_new = beta_two * moment_two + (1.0 - beta_two) * clipped * clipped
    ratio = moment_new / correct_one / (jnp.sqrt(second_new / correct_two) + adam_epsilon)
    param_new = params - learning_rate * (ratio + weight_decay * params)
    out_p = jnp.where(keeping, params, param_new).reshape(row_count, columns)
    out_m = jnp.where(keeping, moment_one, moment_new).reshape(row_count, columns)
    out_v = jnp.where(keeping, moment_two, second_new).reshape(row_count, columns)
    weights = lax.all_gather(out_p.astype(jnp.bfloat16), FSDP, axis=0, tiled=True)
    return out_p, out_m, out_v, weights


def solution(mesh):
    tp = mesh.shape["tp"]
    finer = Mesh(mesh.devices.reshape(8, 4, 2, tp), ALL)
    spec = P(FSDP, "tp")

    def step(*args):
        return local(mesh.devices.size, *args)

    return jax.shard_map(
        step,
        mesh=finer,
        in_specs=(spec, spec, spec, spec, P(), P()),
        out_specs=(spec, spec, spec, P(None, "tp")),
        check_vma=False,
    )
```

```python
import jax
import jax.numpy as jnp
from jax import lax
from jax.experimental import pallas as pl
from jax.experimental.pallas import tpu as pltpu
from jax.sharding import Mesh
from jax.sharding import PartitionSpec as P


ROUNDS = 4
FSDP = ("z", "x", "core")
ALL = ("z", "x", "core", "tp")
Z, X = 8, 4


beta_one = 0.9
beta_two = 0.95
adam_epsilon = 1e-08
learning_rate = 0.01
weight_decay = 0.1
clip_norm = 1.0
square_limit = 1000000.0


def sum_over_devices(value, devices):
    copies = jnp.broadcast_to(value, (devices,) + value.shape)
    return jnp.sum(lax.all_to_all(copies, ALL, 0, 0, tiled=True), axis=0)


def swap(value):
    return lax.ppermute(value, "core", [(0, 1), (1, 0)])


def along(value, axis, size):
    pairs = []
    for i in range(size):
        pairs.append((2 * i, 2 * ((i + 1) % size)))
        pairs.append((2 * i + 1, 2 * ((i - 1) % size) + 1))
    return lax.ppermute(value, (axis, "core"), pairs)


def placer(columns, tile, jobs):
    def kernel(where_ref, *refs):
        z, x, core = where_ref[0], where_ref[1], where_ref[2]
        pieces, out, sems = refs[: len(jobs)], refs[-2], refs[-1]
        copies = []
        for piece, job in zip(pieces, jobs):
            for start, rows, at_z, at_x, sub in job(z, x, core):
                at_z, at_x = lax.rem(at_z + Z, Z), lax.rem(at_x + X, X)
                row = pl.multiple_of((at_z * X + at_x) * (2 * tile) + sub, tile // 2)
                copies.append(
                    pltpu.make_async_copy(
                        piece.at[pl.ds(start, rows)],
                        out.at[pl.ds(row, rows)],
                        sems.at[len(copies)],
                    )
                )
                copies[-1].start()
        for copy in copies:
            copy.wait()

    def count():
        return sum(len(job(0, 0, 0)) for job in jobs)

    def call(where, pieces, into=None):
        extra = [] if into is None else [into]
        return pl.pallas_call(
            kernel,
            out_shape=jax.ShapeDtypeStruct((Z * X * 2 * tile, columns), jnp.bfloat16),
            in_specs=[pl.BlockSpec(memory_space=pltpu.SMEM)]
            + [pl.BlockSpec(memory_space=pl.ANY)] * (len(pieces) + len(extra)),
            out_specs=pl.BlockSpec(memory_space=pl.ANY),
            scratch_shapes=[pltpu.SemaphoreType.DMA((count(),))],
            input_output_aliases={} if into is None else {1 + len(pieces): 0},
            compiler_params=pltpu.CompilerParams(vmem_limit_bytes=1 << 20),
            cost_estimate=pl.CostEstimate(
                flops=1 << 23,
                bytes_accessed=2 * sum(p.size * 2 for p in pieces),
                transcendentals=0,
            ),
        )(where, *pieces, *extra)

    return call


def gather(mine, columns):
    tile = mine.shape[0]
    half = tile // 2
    core = lax.axis_index("core")
    where = jnp.stack([lax.axis_index("z"), lax.axis_index("x"), core]).astype(jnp.int32)

    def cut(value, step, rows):
        return lax.dynamic_slice_in_dim(value, core * step, rows)

    other = swap(mine)
    first = jnp.where(core == 0, mine, other)
    second = jnp.where(core == 0, other, mine)

    a1 = along(first, "x", X)
    e1 = along(second, "z", Z)
    a2 = along(cut(a1, half, half), "x", X)
    s1 = swap(a1)
    e2 = along(e1, "z", Z)
    u1 = swap(e1)
    s2 = swap(a2)
    row = jnp.concatenate([first, a1, a2, s2, s1])
    b1 = along(row, "z", Z)
    e3 = along(e2, "z", Z)
    u2 = swap(e2)
    e4 = along(cut(e3, half, half), "z", Z)
    u3 = swap(e3)
    b2 = along(b1, "z", Z)
    u4 = swap(e4)
    t1 = swap(b1)
    column = jnp.concatenate([second, e1, e2, e3, e4, u4, u1, u2, u3])
    f1 = along(column, "x", X)
    b3 = along(b2, "z", Z)
    t2 = swap(b2)
    b4 = along(cut(b3, tile, 2 * tile), "z", Z)
    t3 = swap(b3)
    f2 = along(cut(f1, tile, 4 * tile), "x", X)
    g1 = swap(f1)
    t4 = swap(b4)
    g2 = swap(f2)

    def whole_row(steps, swapped):
        def job(z, x, core):
            order = 1 - core if swapped else core
            way = 1 - 2 * order
            at = z - way * steps
            return [
                (0, tile, at, x, 0),
                (tile, tile, at, x - way, 0),
                (2 * tile, half, at, x + 2, half * order),
                (2 * tile + half, half, at, x + 2, half * (1 - order)),
                (3 * tile, tile, at, x + way, 0),
            ]

        return job

    def half_row(swapped):
        def job(z, x, core):
            order = 1 - core if swapped else core
            last = x - 1 + 3 * order
            return [
                (0, tile, z + 4, x + order, 0),
                (tile, half, z + 4, last, half * order),
                (tile + half, half, z + 4, last, half * (1 - order)),
            ]

        return job

    def whole_column(steps, swapped):
        def job(z, x, core):
            order = 1 - core if swapped else core
            way = 1 - 2 * order
            at = x - way * steps
            blocks = [(j * tile, tile, z - way * j, at, tile) for j in range(4)]
            blocks += [
                (4 * tile, half, z + 4, at, tile + half * order),
                (4 * tile + half, half, z + 4, at, tile + half * (1 - order)),
            ]
            return blocks + [((4 + j) * tile, tile, z + way * j, at, tile) for j in range(1, 4)]

        return job

    def half_column(swapped):
        def job(z, x, core):
            order = 1 - core if swapped else core
            way = 1 - 2 * order
            last = z - 3 + 7 * order
            blocks = [(j * tile, tile, z - way * (order + j), x + 2, tile) for j in range(3)]
            return blocks + [
                (3 * tile, half, last, x + 2, tile + half * order),
                (3 * tile + half, half, last, x + 2, tile + half * (1 - order)),
            ]

        return job

    early = placer(
        columns,
        tile,
        [whole_row(0, False), whole_row(1, False), whole_row(1, True), whole_column(0, False)],
    )
    late = placer(
        columns,
        tile,
        [
            whole_row(2, False),
            whole_row(2, True),
            whole_row(3, False),
            whole_row(3, True),
            half_row(False),
            half_row(True),
            whole_column(1, False),
            whole_column(1, True),
            half_column(False),
            half_column(True),
        ],
    )
    partly = early(where, [row, b1, t1, column])
    return late(where, [b2, t2, b3, t3, b4, t4, f1, g1, f2, g2], partly)


def local(devices, master, first_moment, second_moment, gradients, step_count, tile_round):
    row_count, columns = master.shape
    shaped = (ROUNDS, row_count // ROUNDS, columns)
    params = master.reshape(shaped)
    moment_one = first_moment.reshape(shaped)
    moment_two = second_moment.reshape(shaped)
    grads = gradients.reshape(shaped)
    mine = lax.dynamic_slice_in_dim(tile_round, lax.axis_index(FSDP) * ROUNDS, ROUNDS)
    is_round = mine[None, :] == jnp.arange(ROUNDS, dtype=jnp.int32)[:, None]
    squares = jnp.sum(grads * grads, axis=(1, 2))
    totals = sum_over_devices(
        jnp.sum(jnp.where(is_round, squares[None, :], 0.0), axis=1), devices
    )
    total_of_slot = jnp.sum(jnp.where(is_round, totals[:, None], 0.0), axis=0)
    total_of_slot = total_of_slot.reshape(ROUNDS, 1, 1)
    scale = jnp.minimum(jnp.float32(1.0), clip_norm / (jnp.sqrt(total_of_slot) + 1e-06))
    keeping = total_of_slot >= square_limit
    steps = step_count[0].astype(jnp.float32)
    correct_one = 1.0 - jnp.power(jnp.float32(beta_one), steps)
    correct_two = 1.0 - jnp.power(jnp.float32(beta_two), steps)
    clipped = grads * scale
    moment_new = beta_one * moment_one + (1.0 - beta_one) * clipped
    second_new = beta_two * moment_two + (1.0 - beta_two) * clipped * clipped
    ratio = moment_new / correct_one / (jnp.sqrt(second_new / correct_two) + adam_epsilon)
    param_new = params - learning_rate * (ratio + weight_decay * params)
    out_p = jnp.where(keeping, params, param_new).reshape(row_count, columns)
    out_m = jnp.where(keeping, moment_one, moment_new).reshape(row_count, columns)
    out_v = jnp.where(keeping, moment_two, second_new).reshape(row_count, columns)
    weights = gather(out_p.astype(jnp.bfloat16), columns)
    return out_p, out_m, out_v, weights


def solution(mesh):
    tp = mesh.shape["tp"]
    finer = Mesh(mesh.devices.reshape(Z, X, 2, tp), ALL)
    spec = P(FSDP, "tp")

    def step(*args):
        return local(mesh.devices.size, *args)

    return jax.shard_map(
        step,
        mesh=finer,
        in_specs=(spec, spec, spec, spec, P(), P()),
        out_specs=(spec, spec, spec, P(None, "tp")),
        check_vma=False,
    )
```

```python
import jax
import jax.numpy as jnp
from jax import lax
from jax.experimental import pallas as pl
from jax.experimental.pallas import tpu as pltpu
from jax.sharding import Mesh
from jax.sharding import PartitionSpec as P


ROUNDS = 4
FSDP = ("z", "x", "core")
ALL = ("z", "x", "core", "tp")
Z, X = 8, 4
VARIANT = {"e": "direct", "f": "ring", "kernels": 2}


beta_one = 0.9
beta_two = 0.95
adam_epsilon = 1e-08
learning_rate = 0.01
weight_decay = 0.1
clip_norm = 1.0
square_limit = 1000000.0


def sum_over_devices(value, devices):
    copies = jnp.broadcast_to(value, (devices,) + value.shape)
    return jnp.sum(lax.all_to_all(copies, ALL, 0, 0, tiled=True), axis=0)


def swap(value):
    return lax.ppermute(value, "core", [(0, 1), (1, 0)])


def along(value, axis, size, steps=1):
    pairs = []
    for i in range(size):
        pairs.append((2 * i, 2 * ((i + steps) % size)))
        pairs.append((2 * i + 1, 2 * ((i - steps) % size) + 1))
    return lax.ppermute(value, (axis, "core"), pairs)


def place(where, group, columns, tile, into):
    def blocks(z, x, core):
        for i, (_, job, swapped) in enumerate(group):
            order = 1 - core if swapped else core
            for block in job(z, x, order, 1 - 2 * order):
                yield i, block

    def kernel(where_ref, *refs):
        out, sems = refs[-2], refs[-1]
        copies = []
        for i, (start, rows, at_z, at_x, sub) in blocks(where_ref[0], where_ref[1], where_ref[2]):
            at_z, at_x = lax.rem(at_z + Z, Z), lax.rem(at_x + X, X)
            row = pl.multiple_of((at_z * X + at_x) * (2 * tile) + sub, tile // 2)
            copy = pltpu.make_async_copy(
                refs[i].at[pl.ds(start, rows)], out.at[pl.ds(row, rows)], sems.at[len(copies)]
            )
            copy.start()
            copies.append(copy)
        for copy in copies:
            copy.wait()

    pieces = [piece for piece, _, _ in group]
    extra = [] if into is None else [into]
    return pl.pallas_call(
        kernel,
        out_shape=jax.ShapeDtypeStruct((Z * X * 2 * tile, columns), jnp.bfloat16),
        in_specs=[pl.BlockSpec(memory_space=pltpu.SMEM)]
        + [pl.BlockSpec(memory_space=pl.ANY)] * (len(pieces) + len(extra)),
        out_specs=pl.BlockSpec(memory_space=pl.ANY),
        scratch_shapes=[pltpu.SemaphoreType.DMA((len(list(blocks(0, 0, 0))),))],
        input_output_aliases={} if into is None else {1 + len(pieces): 0},
        compiler_params=pltpu.CompilerParams(vmem_limit_bytes=1 << 20),
        cost_estimate=pl.CostEstimate(
            flops=1 << 20, bytes_accessed=4 * sum(p.size for p in pieces), transcendentals=0
        ),
    )(where, *pieces, *extra)


def gather(mine, columns, variant=VARIANT):
    tile = mine.shape[0]
    half = tile // 2
    core = lax.axis_index("core")
    where = jnp.stack([lax.axis_index("z"), lax.axis_index("x"), core]).astype(jnp.int32)
    where, mine = lax.optimization_barrier((where, mine))
    ahead = core == 0
    join = jnp.concatenate

    other = swap(mine)
    first = jnp.where(ahead, mine, other)
    second = jnp.where(ahead, other, mine)

    def part(value):
        return jnp.where(ahead, value[:half], value[half:])

    a1 = along(first, "x", X)
    a2 = along(part(first), "x", X, 2)
    e1 = along(second, "z", Z)
    e2 = along(second, "z", Z, 2)
    if variant["e"] == "direct":
        e3 = along(second, "z", Z, 3)
        e4 = along(part(second), "z", Z, 4)
    else:
        e3 = along(e1, "z", Z, 2)
        e4 = along(part(e2), "z", Z, 2)
    row_near = join([first, a1])
    s = swap(join([a1, a2]))
    row_far = join([a2, s[tile:], s[:tile]])
    column_near = join([second, e1, e2, e3])
    u = swap(join([e1, e2, e3, e4]))
    column_far = join([e4, u[3 * tile :], u[: 3 * tile]])

    b1n = along(row_near, "z", Z)
    f1n = along(column_near, "x", X)
    b1f = along(row_far, "z", Z)
    f1f = along(column_far, "x", X)
    b2n = along(b1n, "z", Z)
    b2f = along(b1f, "z", Z)
    b3n = along(b2n, "z", Z)
    b3f = along(b2f, "z", Z)
    if variant["f"] == "ring":
        f2 = along(jnp.where(ahead, f1n, join([f1n[tile:], f1f[:tile]])), "x", X)
    else:
        f2 = along(jnp.where(ahead, column_near, join([column_near[tile:], column_far[:tile]])), "x", X, 2)
    b4 = along(jnp.where(ahead, b3n, join([b3n[tile:], b3f[:tile]])), "z", Z)

    def near_row(steps):
        def job(z, x, order, way):
            at = z - way * steps
            return [(0, tile, at, x, 0), (tile, tile, at, x - way, 0)]

        return job

    def far_row(steps):
        def job(z, x, order, way):
            at = z - way * steps
            return [
                (0, half, at, x + 2, half * order),
                (half, half, at, x + 2, half * (1 - order)),
                (tile, tile, at, x + way, 0),
            ]

        return job

    def across_row(z, x, order, way):
        last = x - 1 + 3 * order
        return [
            (0, tile, z + 4, x + order, 0),
            (tile, half, z + 4, last, half * order),
            (tile + half, half, z + 4, last, half * (1 - order)),
        ]

    def near_column(steps):
        def job(z, x, order, way):
            return [(j * tile, tile, z - way * j, x - way * steps, tile) for j in range(4)]

        return job

    def far_column(steps):
        def job(z, x, order, way):
            at = x - way * steps
            return [
                (0, half, z + 4, at, tile + half * order),
                (half, half, z + 4, at, tile + half * (1 - order)),
            ] + [(j * tile, tile, z + way * j, at, tile) for j in range(1, 4)]

        return job

    def across_column(z, x, order, way):
        last = z - 3 + 7 * order
        return [(j * tile, tile, z - way * (order + j), x + 2, tile) for j in range(3)] + [
            (3 * tile, half, last, x + 2, tile + half * order),
            (3 * tile + half, half, last, x + 2, tile + half * (1 - order)),
        ]

    def both(pieces):
        return [(p, job, False) for p, job in pieces] + [(swap(p), job, True) for p, job in pieces]

    own = [(row_near, near_row(0)), (row_far, far_row(0)), (column_near, near_column(0)), (column_far, far_column(0))]
    groups = [
        [(p, job, False) for p, job in own] + both([(b1n, near_row(1)), (b1f, far_row(1))]),
        both([(b2n, near_row(2)), (b2f, far_row(2)), (f1n, near_column(1)), (f1f, far_column(1))]),
        both([(b3n, near_row(3)), (b3f, far_row(3)), (f2, across_column), (b4, across_row)]),
    ]
    if variant["kernels"] == 2:
        groups = [groups[0], groups[1] + groups[2]]
    out = None
    for group in groups:
        out = place(where, group, columns, tile, out)
    return out


def local(devices, master, first_moment, second_moment, gradients, step_count, tile_round):
    row_count, columns = master.shape
    shaped = (ROUNDS, row_count // ROUNDS, columns)
    params = master.reshape(shaped)
    moment_one = first_moment.reshape(shaped)
    moment_two = second_moment.reshape(shaped)
    grads = gradients.reshape(shaped)
    mine = lax.dynamic_slice_in_dim(tile_round, lax.axis_index(FSDP) * ROUNDS, ROUNDS)
    is_round = mine[None, :] == jnp.arange(ROUNDS, dtype=jnp.int32)[:, None]
    squares = jnp.sum(grads * grads, axis=(1, 2))
    totals = sum_over_devices(
        jnp.sum(jnp.where(is_round, squares[None, :], 0.0), axis=1), devices
    )
    total_of_slot = jnp.sum(jnp.where(is_round, totals[:, None], 0.0), axis=0)
    total_of_slot = total_of_slot.reshape(ROUNDS, 1, 1)
    scale = jnp.minimum(jnp.float32(1.0), clip_norm / (jnp.sqrt(total_of_slot) + 1e-06))
    keeping = total_of_slot >= square_limit
    steps = step_count[0].astype(jnp.float32)
    correct_one = 1.0 - jnp.power(jnp.float32(beta_one), steps)
    correct_two = 1.0 - jnp.power(jnp.float32(beta_two), steps)
    clipped = grads * scale
    moment_new = beta_one * moment_one + (1.0 - beta_one) * clipped
    second_new = beta_two * moment_two + (1.0 - beta_two) * clipped * clipped
    ratio = moment_new / correct_one / (jnp.sqrt(second_new / correct_two) + adam_epsilon)
    param_new = params - learning_rate * (ratio + weight_decay * params)
    out_p = jnp.where(keeping, params, param_new).reshape(row_count, columns)
    out_m = jnp.where(keeping, moment_one, moment_new).reshape(row_count, columns)
    out_v = jnp.where(keeping, moment_two, second_new).reshape(row_count, columns)
    weights = gather(out_p.astype(jnp.bfloat16), columns)
    return out_p, out_m, out_v, weights


def solution(mesh):
    tp = mesh.shape["tp"]
    finer = Mesh(mesh.devices.reshape(Z, X, 2, tp), ALL)
    spec = P(FSDP, "tp")

    def step(*args):
        return local(mesh.devices.size, *args)

    return jax.shard_map(
        step,
        mesh=finer,
        in_specs=(spec, spec, spec, spec, P(), P()),
        out_specs=(spec, spec, spec, P(None, "tp")),
        check_vma=False,
    )
```
